32 devices in a mesh: groups: 2 (over y), seq: 16 (over z, x, core).
Axes of the slice: x: 2, y: 2, z: 4, core: 2. Of those that a mesh axis runs over, the one named last changes fastest.
Arguments:
- queries: bfloat16 [8192, 2048], P(('groups', 'seq')), parts along dimension 0, may hold values from -20 to 20
- keys: bfloat16 [8192, 2048], P(('groups', 'seq')), parts along dimension 0, may hold values from -20 to 20
- values: bfloat16 [8192, 2048], P(('groups', 'seq')), parts along dimension 0, may hold values from -6 to 6
- block_counts: int32 [16], P('groups'), parts along dimension 0, may hold values from 2 to 6, as said below
- last_tokens: int32 [32], P('groups'), parts along dimension 0, may hold values from 64 to 128
- pack_order: int32 [32], P('groups'), parts along dimension 0, may hold values from 0 to 15, as said below
- decode_slot: int32 [16], P('groups'), parts along dimension 0, may hold values from 0 to 7, each once
Outputs:
- attended: bfloat16 [8192, 2048], P(('groups', 'seq')), parts along dimension 0
- cache_keys: bfloat16 [32, 32, 128, 128], P(('groups', 'seq')), parts along dimension 0
- cache_values: bfloat16 [32, 32, 128, 128], P(('groups', 'seq')), parts along dimension 0
The draws below stay inside these ranges and needn't reach their ends.
There are 2 independent parts, one for each index of `groups`. The reference program is written for one: setup_inputs(seed, part) draws one part's arguments, and reference() takes and returns one part's arrays. A program takes and returns all parts, laid end to end along the dimension named above; each array names one. Nothing has to cross between parts.
Inputs may be any that keep to these rules, and one draw needn't show every extreme that they name: `block_counts`: they sum to 24; the largest equals 6. `pack_order`: each prompt number appears once. The last 1 positions hold null prompts, and the position before them a conditional prompt of 6 blocks. `decode_slot`: each slot appears once.
All inputs are finite; a program needn't handle non-finite values.
Results may differ from the reference program's by a relative error of at most 0.0034.
Values may be sent and summed in bfloat16 or wider, within the bound.
No kernel may reach another device: no remote copies, remote signals or barrier semaphores. Data moves between devices by JAX's collectives and lax.ppermute only.
A program may use at most 64 MiB of HBM per device.

```python
import jax
import jax.numpy as jnp
from jax import lax

HEADS = 16
HEAD_DIM = 128
BLOCK = 128
MAXB = 6
BLK_DEV = 2
NB = 32
TOKENS = 4096
PAIRS = 8
SPLITS = 1
SLICE = 128


def draw_queries(key, part):
    noise = jnp.clip(jax.random.normal(jax.random.fold_in(key, 1), (TOKENS, HEADS * HEAD_DIM), jnp.float32), -6.0, 6.0)
    return noise.astype(jnp.bfloat16)


def draw_keys(key, part):
    noise = jnp.clip(jax.random.normal(jax.random.fold_in(key, 2), (TOKENS, HEADS * HEAD_DIM), jnp.float32), -6.0, 6.0)
    return noise.astype(jnp.bfloat16)


def pack_plan(key):
    base = jax.random.fold_in(key, 11)
    first_key, second_key, third_key, fourth_key = jax.random.split(base, 4)
    pair_ids = jnp.arange(PAIRS, dtype=jnp.int32)
    biggest = jax.random.randint(first_key, (), 0, PAIRS).astype(jnp.int32)
    counts = jnp.where(pair_ids == biggest, MAXB, 2).astype(jnp.int32)
    extra = NB - PAIRS - (2 * (PAIRS - 1) + MAXB)

    def add_one(step, current):
        scores = jax.random.randint(jax.random.fold_in(second_key, step), (PAIRS,), 0, 1 << 20).astype(jnp.int32) * PAIRS + pair_ids
        scores = jnp.where(current < MAXB, scores, -1)
        chosen = jnp.argmax(scores).astype(jnp.int32)
        return current + (pair_ids == chosen).astype(jnp.int32)
    counts = lax.fori_loop(0, extra, add_one, counts)
    null_order = jax.random.permutation(third_key, PAIRS).astype(jnp.int32)
    tail_nulls = PAIRS + null_order[:BLK_DEV - 1]
    spare_nulls = PAIRS + null_order[BLK_DEV - 1:]
    spare_count = PAIRS - BLK_DEV + 1
    cond_order = jax.random.permutation(fourth_key, PAIRS).astype(jnp.int32)
    rank_keys = jnp.where(cond_order == biggest, PAIRS, pair_ids).astype(jnp.int32)
    cond_seq = cond_order[jnp.argsort(rank_keys, stable=True)][:PAIRS - 1]
    first_edge = BLK_DEV
    middle_edge = NB // BLK_DEV // 2 * BLK_DEV
    order = jnp.zeros((2 * PAIRS,), jnp.int32)

    def place(step, carry):
        current, write, start, queue = carry
        prompt = cond_seq[step]
        size = counts[prompt]
        filler = (start + size == first_edge) | (start + size == middle_edge)
        current = current.at[write].set(jnp.where(filler, spare_nulls[queue], prompt))
        bump = filler.astype(jnp.int32)
        write = write + bump
        start = start + bump
        queue = queue + bump
        current = current.at[write].set(prompt)
        return (current, write + 1, start + size, queue)
    zero = jnp.zeros((), jnp.int32)
    order, write, start, queue = lax.fori_loop(0, PAIRS - 1, place, (order, zero, zero, zero))

    def rest(index, current):
        keep = index >= queue
        target = jnp.where(keep, write + index - queue, 2 * PAIRS - 1).astype(jnp.int32)
        return current.at[target].set(jnp.where(keep, spare_nulls[index], current[target]))
    order = lax.fori_loop(0, spare_count, rest, order)
    order = order.at[2 * PAIRS - BLK_DEV].set(biggest)
    order = order.at[2 * PAIRS - BLK_DEV + 1:].set(tail_nulls)
    return (counts, order.astype(jnp.int32))


def draw_block_counts(key, part):
    counts, order = pack_plan(key)
    return counts


def draw_pack_order(key, part):
    counts, order = pack_plan(key)
    return order


def touch_ends(array, rng, smallest, high):
    shape = array.shape
    spot = [jax.random.randint(jax.random.fold_in(rng, axis), (), 0, shape[axis]) for axis in range(len(shape))]
    array = array.at[tuple(spot)].set(smallest)
    longest = shape.index(max(shape))
    spot[longest] = (spot[longest] + 1) % shape[longest]
    return array.at[tuple(spot)].set(high)


def levels(rng, shape, cuts, smallest, largest):
    factor_of = 1.0
    for dim, parts in cuts:
        draws = jax.random.uniform(jax.random.fold_in(jax.random.fold_in(rng, 6), dim), (parts,), jnp.float32, smallest / len(cuts), largest / len(cuts))
        factor_of = factor_of * jnp.repeat(jnp.exp(draws), shape[dim] // parts).reshape((-1,) + (1,) * (len(shape) - 1 - dim))
    return factor_of


def bell_draw(rng, shape, scale, reach, cuts=(), kind=jnp.bfloat16):
    factor_of = levels(rng, shape, cuts, -0.22, 0.18) if cuts else 1.0
    array = jax.random.normal(rng, shape, jnp.float32) * scale * factor_of
    return jnp.minimum(jnp.maximum(array, -reach), reach).astype(kind)


def setup_inputs(seed: int = 0, part: int = 0) -> dict:
    splits = jax.random.split(jax.random.key(seed), 8)
    own_keys = jax.random.split(jax.random.fold_in(splits[7], part), 8)
    queries = draw_queries(jax.random.fold_in(jax.random.fold_in(splits[7], part), 71), part)
    keys = draw_keys(jax.random.fold_in(jax.random.fold_in(splits[7], part), 71), part)
    values = bell_draw(own_keys[2], (TOKENS, HEADS * HEAD_DIM), 1.0, 6.0, ((0, 16),))
    block_counts = draw_block_counts(jax.random.fold_in(jax.random.fold_in(splits[7], part), 71), part)
    last_tokens = touch_ends(jax.random.randint(own_keys[4], (2 * PAIRS,), BLOCK // 2, BLOCK + 1), jax.random.fold_in(own_keys[4], 1), BLOCK // 2, BLOCK).astype(jnp.int32)
    pack_order = draw_pack_order(jax.random.fold_in(jax.random.fold_in(splits[7], part), 71), part)
    decode_slot = jax.random.permutation(own_keys[6], PAIRS).astype(jnp.int32)
    return {"queries": queries, "keys": keys, "values": values, "block_counts": block_counts, "last_tokens": last_tokens, "pack_order": pack_order, "decode_slot": decode_slot}


MASKED_SCORE = -1.0e30


def block_tables(block_counts, last_tokens, pack_order, decode_slot, total_blocks, block):
    pair_count = block_counts.shape[0]
    prompts = 2 * pair_count
    prompt_ids = jnp.arange(prompts, dtype=jnp.int32)
    prompt_sizes = jnp.concatenate([block_counts, jnp.ones((pair_count,), jnp.int32)])
    picked = (pack_order[:, None] == prompt_ids[None, :]).astype(jnp.int32)
    packed_sizes = jnp.sum(picked * prompt_sizes[None, :], axis=1).astype(jnp.int32)
    packed_tails = jnp.sum(picked * last_tokens[None, :], axis=1).astype(jnp.int32)
    block_ends = jnp.cumsum(packed_sizes).astype(jnp.int32)
    starts = block_ends - packed_sizes
    blocks = jnp.arange(total_blocks, dtype=jnp.int32)
    member = ((starts[None, :] <= blocks[:, None]) & (blocks[:, None] < block_ends[None, :])).astype(jnp.int32)
    position = jnp.sum(member * prompt_ids[None, :], axis=1).astype(jnp.int32)
    prompt = jnp.sum(member * pack_order[None, :], axis=1).astype(jnp.int32)
    within = blocks - jnp.sum(member * starts[None, :], axis=1).astype(jnp.int32)
    is_last = (blocks + 1) == jnp.sum(member * block_ends[None, :], axis=1).astype(jnp.int32)
    valid_tokens = jnp.where(is_last, jnp.sum(member * packed_tails[None, :], axis=1).astype(jnp.int32), block).astype(jnp.int32)
    pair_ids = jnp.arange(pair_count, dtype=jnp.int32)
    earlier = (decode_slot[None, :] < decode_slot[:, None]).astype(jnp.int32)
    slot_start = jnp.sum(earlier * (block_counts + 1)[None, :], axis=1).astype(jnp.int32)
    pair_of = prompt % pair_count
    owner = (pair_of[:, None] == pair_ids[None, :]).astype(jnp.int32)
    base_slot = jnp.sum(owner * slot_start[None, :], axis=1).astype(jnp.int32)
    own_count = jnp.sum(owner * block_counts[None, :], axis=1).astype(jnp.int32)
    destination = base_slot + jnp.where(prompt >= pair_count, own_count, within)
    hits = (destination[None, :] == blocks[:, None]).astype(jnp.int32)
    source = jnp.sum(hits * blocks[None, :], axis=1).astype(jnp.int32)
    return position, valid_tokens, source


def reference(queries, keys, values, block_counts, last_tokens, pack_order, decode_slot):
    position, valid_tokens, source = block_tables(block_counts, last_tokens, pack_order, decode_slot, NB, BLOCK)
    features = HEADS * HEAD_DIM
    back = MAXB - 1
    span = (back + 1) * BLOCK
    padding = jnp.zeros((back * BLOCK, features), jnp.bfloat16)
    padded_keys = jnp.concatenate([padding, keys], axis=0)
    padded_values = jnp.concatenate([padding, values], axis=0)
    padded_docs = jnp.concatenate([jnp.full((back,), -1, jnp.int32), position])
    padded_valid = jnp.concatenate([jnp.zeros((back,), jnp.int32), valid_tokens])
    token_ids = jnp.arange(BLOCK, dtype=jnp.int32)
    key_blocks = jnp.repeat(jnp.arange(back + 1, dtype=jnp.int32), BLOCK)
    key_tokens = jnp.tile(token_ids, back + 1)
    score_scale = HEAD_DIM ** -0.5

    def one_block(block_index):
        start = (block_index * BLOCK).astype(jnp.int32)
        key_window = lax.dynamic_slice_in_dim(padded_keys, start, span, 0).reshape(span, HEADS, HEAD_DIM)
        value_window = lax.dynamic_slice_in_dim(padded_values, start, span, 0).reshape(span, HEADS, HEAD_DIM)
        window_docs = lax.dynamic_slice_in_dim(padded_docs, block_index, back + 1)
        window_valid = lax.dynamic_slice_in_dim(padded_valid, block_index, back + 1)
        query_block = lax.dynamic_slice_in_dim(queries, start, BLOCK, 0).reshape(BLOCK, HEADS, HEAD_DIM)
        own_doc = window_docs[back]
        own_valid = window_valid[back]
        key_ok = (jnp.repeat(window_docs, BLOCK) == own_doc) & (key_tokens < jnp.repeat(window_valid, BLOCK))
        causal = (key_blocks[None, :] < back) | (key_tokens[None, :] <= token_ids[:, None])
        allowed = causal & key_ok[None, :]
        scores = jnp.einsum("qhd,khd->hqk", query_block.astype(jnp.float32), key_window.astype(jnp.float32)) * score_scale
        scores = jnp.where(allowed[None], scores, MASKED_SCORE)
        peak = jnp.max(scores, axis=2, keepdims=True)
        weights = jnp.exp(scores - peak)
        totals = jnp.sum(weights, axis=2, keepdims=True)
        rounded = lax.optimization_barrier(weights.astype(jnp.bfloat16)).astype(jnp.float32)
        mixed = jnp.einsum("hqk,khd->hqd", rounded, value_window.astype(jnp.float32)) / totals
        mixed = jnp.where((token_ids < own_valid)[None, :, None], mixed, 0.0)
        return jnp.transpose(mixed, (1, 0, 2)).reshape(BLOCK, features).astype(jnp.bfloat16)

    attended = lax.map(one_block, jnp.arange(NB, dtype=jnp.int32)).reshape(TOKENS, features)

    def relayout(source_array):
        grid = source_array.reshape(NB, SPLITS, SLICE, HEADS, HEAD_DIM)
        reordered = jnp.take(grid, source, axis=0)
        return jnp.transpose(reordered, (3, 1, 0, 2, 4)).reshape(HEADS * SPLITS, NB, SLICE, HEAD_DIM)

    return attended, relayout(keys), relayout(values)
```

```python
import jax
import jax.numpy as jnp
from jax import lax
from jax.experimental import pallas as pl
from jax.experimental.pallas import tpu as pltpu
from jax.sharding import PartitionSpec as P

HEADS = 16
HEAD_DIM = 128
BLOCK = 128
MAXB = 6


MASKED_SCORE = -1e30


HEADS_STEP = 2
CHUNK = 32


def sent(block, pairs):
    return lax.ppermute(block, "seq", pairs)


def block_tables(block_counts, last_tokens, pack_order, decode_slot, total_blocks, block):
    pair_count = block_counts.shape[0]
    prompts = 2 * pair_count
    prompt_ids = jnp.arange(prompts, dtype=jnp.int32)
    prompt_sizes = jnp.concatenate([block_counts, jnp.ones((pair_count,), jnp.int32)])
    picked = (pack_order[:, None] == prompt_ids[None, :]).astype(jnp.int32)
    packed_sizes = jnp.sum(picked * prompt_sizes[None, :], axis=1)
    packed_tails = jnp.sum(picked * last_tokens[None, :], axis=1)
    block_ends = jnp.cumsum(packed_sizes)
    starts = block_ends - packed_sizes
    blocks = jnp.arange(total_blocks, dtype=jnp.int32)
    member = (
        (starts[None, :] <= blocks[:, None]) & (blocks[:, None] < block_ends[None, :])
    ).astype(jnp.int32)
    prompt = jnp.sum(member * pack_order[None, :], axis=1)
    within = blocks - jnp.sum(member * starts[None, :], axis=1)
    is_last = blocks + 1 == jnp.sum(member * block_ends[None, :], axis=1)
    valid_tokens = jnp.where(is_last, jnp.sum(member * packed_tails[None, :], axis=1), block)
    pair_ids = jnp.arange(pair_count, dtype=jnp.int32)
    earlier = (decode_slot[None, :] < decode_slot[:, None]).astype(jnp.int32)
    slot_start = jnp.sum(earlier * (block_counts + 1)[None, :], axis=1)
    pair_of = prompt % pair_count
    owner = (pair_of[:, None] == pair_ids[None, :]).astype(jnp.int32)
    base_slot = jnp.sum(owner * slot_start[None, :], axis=1)
    own_count = jnp.sum(owner * block_counts[None, :], axis=1)
    destination = base_slot + jnp.where(prompt >= pair_count, own_count, within)
    hits = (destination[None, :] == blocks[:, None]).astype(jnp.int32)
    source = jnp.sum(hits * blocks[None, :], axis=1)
    return (within, valid_tokens, source)


def pack_kernel(keys, values, out):
    splits, _, blocks_here, slice_len, _ = out.shape
    for which, ref in enumerate((keys, values)):
        for b in range(blocks_here):
            for t in range(splits):
                first = b * BLOCK + t * slice_len
                out[t, which, b] = ref[first : first + slice_len, :]


def packed(keys, values, splits):
    tokens_here = keys.shape[0]
    blocks_here = tokens_here // BLOCK
    slice_len = BLOCK // splits
    piece = (splits, 2, blocks_here, slice_len, HEAD_DIM)
    spec = pl.BlockSpec((tokens_here, HEAD_DIM), lambda h: (0, h))
    return pl.pallas_call(
        pack_kernel,
        grid=(HEADS,),
        in_specs=[spec, spec],
        out_specs=pl.BlockSpec(piece, lambda h: (h, 0, 0, 0, 0)),
        out_shape=jax.ShapeDtypeStruct((HEADS * splits,) + piece[1:], keys.dtype),
    )(keys, values)


def order_kernel(source, arrived, cache_keys, cache_values, sems):
    blocks_here = arrived.shape[2]
    total = cache_keys.shape[1]
    wave = sems.shape[0]

    def copies(start, i):
        block = source[start + i]
        device = block // blocks_here
        local_block = block % blocks_here
        return [
            pltpu.make_async_copy(
                arrived.at[device, which, local_block], out.at[0, start + i], sems.at[i, which]
            )
            for which, out in enumerate((cache_keys, cache_values))
        ]

    def one_wave(step, carry):
        for i in range(wave):
            for copy in copies(step * wave, i):
                copy.start()
        for i in range(wave):
            for copy in copies(step * wave, i):
                copy.wait()
        return carry

    lax.fori_loop(0, total // wave, one_wave, 0)


def ordered(arrived, source):
    total = source.shape[0]
    wave = min(CHUNK, total)
    shape = jax.ShapeDtypeStruct((1, total) + arrived.shape[3:], arrived.dtype)
    anywhere = pl.BlockSpec(memory_space=pl.ANY)
    return pl.pallas_call(
        order_kernel,
        grid_spec=pltpu.PrefetchScalarGridSpec(
            num_scalar_prefetch=1,
            grid=(1,),
            in_specs=[anywhere],
            out_specs=[anywhere, anywhere],
            scratch_shapes=[pltpu.SemaphoreType.DMA((wave, 2))],
        ),
        out_shape=[shape, shape],
    )(source, arrived)


def attend_kernel(info, q, *refs):
    key_refs, value_refs, out = refs[:5], refs[5:10], refs[10]
    odd = info[0] == 1

    def block_of(group, index, lanes):
        far, two, swapped, near, own = group
        lo, hi = slice(0, BLOCK), slice(BLOCK, 2 * BLOCK)
        rows = hi if index % 2 == 0 else lo
        if index == 0:
            return jnp.where(odd, swapped[hi, lanes], far[:, lanes])
        if index <= 2:
            return two[rows, lanes]
        if index <= 4:
            return jnp.where(odd, near[rows, lanes], swapped[rows, lanes])
        return own[rows, lanes]

    row = lax.broadcasted_iota(jnp.int32, (BLOCK, BLOCK), 0)
    col = lax.broadcasted_iota(jnp.int32, (BLOCK, BLOCK), 1)
    scale = HEAD_DIM ** (-0.5) * 1.4426950408889634

    def one(head, query_block, prior):
        lanes = slice(head * HEAD_DIM, (head + 1) * HEAD_DIM)
        rows = slice(query_block * BLOCK, (query_block + 1) * BLOCK)
        last = MAXB - 1 + query_block
        valid = info[3 + query_block]
        query = q[rows, lanes]
        window = range(last - prior, last + 1)
        parts = [
            lax.dot_general(
                query,
                block_of(key_refs, j, lanes),
                (((1,), (1,)), ((), ())),
                preferred_element_type=jnp.float32,
            )
            for j in window
        ]
        parts[-1] = jnp.where((col <= row) & (col < valid), parts[-1], MASKED_SCORE)
        best = parts[0]
        for part in parts[1:]:
            best = jnp.maximum(best, part)
        peak = jnp.max(best, axis=1, keepdims=True)
        weights = [jnp.exp2((part - peak) * scale) for part in parts]
        summed = weights[0]
        for part in weights[1:]:
            summed = summed + part
        totals = jnp.sum(summed, axis=1, keepdims=True)
        mixed = jnp.zeros((BLOCK, HEAD_DIM), jnp.float32)
        for j, part in zip(window, weights):
            mixed = mixed + jnp.dot(
                part.astype(jnp.bfloat16),
                block_of(value_refs, j, lanes),
                preferred_element_type=jnp.float32,
            )
        result = jnp.where(row < valid, mixed / totals, 0.0)
        out[rows, lanes] = result.astype(jnp.bfloat16)

    for query_block in range(2):
        for prior in range(MAXB):

            @pl.when(info[1 + query_block] == prior)
            def _():
                for head in range(HEADS_STEP):
                    one(head, query_block, prior)


def attend(info, queries, key_parts, value_parts):
    width = HEADS_STEP * HEAD_DIM
    tokens_here, features = queries.shape
    half = tokens_here // 2
    whole = pl.BlockSpec((tokens_here, width), lambda h, info: (0, h))
    far = pl.BlockSpec((half, width), lambda h, info: (0, h * (1 - info[0])))
    near = pl.BlockSpec((tokens_here, width), lambda h, info: (0, h * info[0]))
    group = [far, whole, whole, near, whole]
    return pl.pallas_call(
        attend_kernel,
        grid_spec=pltpu.PrefetchScalarGridSpec(
            num_scalar_prefetch=1,
            grid=(features // width,),
            in_specs=[whole] + group + group,
            out_specs=whole,
        ),
        out_shape=jax.ShapeDtypeStruct(queries.shape, jnp.bfloat16),
        cost_estimate=pl.CostEstimate(
            flops=4 * tokens_here * MAXB * BLOCK * features,
            transcendentals=0,
            bytes_accessed=10 * tokens_here * features,
        ),
    )(info, queries, *key_parts, *value_parts)


def window_parts(own, devices):
    by_two = [(i, i + 2) for i in range(devices - 2)]
    by_three = [(i, i + 3) for i in range(1, devices - 3, 2)]
    to_odd = [(i, i + 1) for i in range(0, devices, 2)]
    exchange = [(i, i ^ 1) for i in range(devices)]
    two = sent(own, by_two)
    far = sent(own[BLOCK:], by_three)
    near = sent(own, to_odd)
    swapped = sent(two, exchange)
    return [far, two, swapped, near, own]


def local(queries, keys, values, block_counts, last_tokens, pack_order, decode_slot):
    devices = lax.axis_size("seq")
    own_index = lax.axis_index("seq")
    blocks_here = queries.shape[0] // BLOCK
    assert blocks_here == 2 and devices % 2 == 0
    splits = devices // HEADS
    within, valid_tokens, source = block_tables(
        block_counts, last_tokens, pack_order, decode_slot, blocks_here * devices, BLOCK
    )
    key_parts = window_parts(keys, devices)
    value_parts = window_parts(values, devices)
    arrived = lax.all_to_all(
        packed(keys, values, splits), "seq", split_axis=0, concat_axis=0, tiled=True
    )
    first = own_index * blocks_here
    info = jnp.concatenate(
        [
            (own_index % 2)[None].astype(jnp.int32),
            lax.dynamic_slice_in_dim(within, first, blocks_here),
            lax.dynamic_slice_in_dim(valid_tokens, first, blocks_here),
        ]
    )
    attended = attend(info, queries, key_parts, value_parts)
    cache_keys, cache_values = ordered(arrived, source)
    return (attended, cache_keys, cache_values)


def solution(mesh):
    placed = (
        P(("groups", "seq"), None),
        P(("groups", "seq"), None),
        P(("groups", "seq"), None),
        P("groups"),
        P("groups"),
        P("groups"),
        P("groups"),
    )
    return jax.shard_map(
        local,
        mesh=mesh,
        in_specs=placed,
        out_specs=(
            P(("groups", "seq"), None),
            P(("groups", "seq"), None, None, None),
            P(("groups", "seq"), None, None, None),
        ),
        check_vma=False,
    )
```

```python
import jax
import jax.numpy as jnp
from jax import lax
from jax.experimental import pallas as pl
from jax.experimental.pallas import tpu as pltpu
from jax.sharding import PartitionSpec as P

HEADS = 16
HEAD_DIM = 128
BLOCK = 128
MAXB = 6


MASKED_SCORE = -1e30


HEADS_STEP = 4
HEADS_PACK = 4


def sent(block, pairs):
    return lax.ppermute(block, "seq", pairs)


def block_tables(block_counts, last_tokens, pack_order, decode_slot, total_blocks, block):
    pair_count = block_counts.shape[0]
    prompts = 2 * pair_count
    prompt_ids = jnp.arange(prompts, dtype=jnp.int32)
    prompt_sizes = jnp.concatenate([block_counts, jnp.ones((pair_count,), jnp.int32)])
    picked = (pack_order[:, None] == prompt_ids[None, :]).astype(jnp.int32)
    packed_sizes = jnp.sum(picked * prompt_sizes[None, :], axis=1)
    packed_tails = jnp.sum(picked * last_tokens[None, :], axis=1)
    block_ends = jnp.cumsum(packed_sizes)
    starts = block_ends - packed_sizes
    blocks = jnp.arange(total_blocks, dtype=jnp.int32)
    member = (
        (starts[None, :] <= blocks[:, None]) & (blocks[:, None] < block_ends[None, :])
    ).astype(jnp.int32)
    prompt = jnp.sum(member * pack_order[None, :], axis=1)
    within = blocks - jnp.sum(member * starts[None, :], axis=1)
    is_last = blocks + 1 == jnp.sum(member * block_ends[None, :], axis=1)
    valid_tokens = jnp.where(is_last, jnp.sum(member * packed_tails[None, :], axis=1), block)
    pair_ids = jnp.arange(pair_count, dtype=jnp.int32)
    earlier = (decode_slot[None, :] < decode_slot[:, None]).astype(jnp.int32)
    slot_start = jnp.sum(earlier * (block_counts + 1)[None, :], axis=1)
    pair_of = prompt % pair_count
    owner = (pair_of[:, None] == pair_ids[None, :]).astype(jnp.int32)
    base_slot = jnp.sum(owner * slot_start[None, :], axis=1)
    own_count = jnp.sum(owner * block_counts[None, :], axis=1)
    destination = base_slot + jnp.where(prompt >= pair_count, own_count, within)
    hits = (destination[None, :] == blocks[:, None]).astype(jnp.int32)
    source = jnp.sum(hits * blocks[None, :], axis=1)
    return (within, valid_tokens, source)


def pack_kernel(keys, values, out):
    rows, _, blocks_here, slice_len, _ = out.shape
    splits = rows // HEADS_PACK
    for which, ref in enumerate((keys, values)):
        for h in range(HEADS_PACK):
            lanes = slice(h * HEAD_DIM, (h + 1) * HEAD_DIM)
            for b in range(blocks_here):
                for t in range(splits):
                    first = b * BLOCK + t * slice_len
                    out[h * splits + t, which, b] = ref[first : first + slice_len, lanes]


def packed(keys, values, splits):
    tokens_here = keys.shape[0]
    blocks_here = tokens_here // BLOCK
    slice_len = BLOCK // splits
    piece = (HEADS_PACK * splits, 2, blocks_here, slice_len, HEAD_DIM)
    spec = pl.BlockSpec((tokens_here, HEADS_PACK * HEAD_DIM), lambda h: (0, h))
    return pl.pallas_call(
        pack_kernel,
        grid=(HEADS // HEADS_PACK,),
        in_specs=[spec, spec],
        out_specs=pl.BlockSpec(piece, lambda h: (h, 0, 0, 0, 0)),
        out_shape=jax.ShapeDtypeStruct((HEADS * splits,) + piece[1:], keys.dtype),
    )(keys, values)


def order_kernel(source, arrived, cache_keys, cache_values, sem):
    blocks_here = arrived.shape[2]
    total = cache_keys.shape[1]

    def start(slot, carry):
        block = source[slot]
        for which, out in enumerate((cache_keys, cache_values)):
            pltpu.make_async_copy(
                arrived.at[block // blocks_here, which, block % blocks_here],
                out.at[0, slot],
                sem.at[which],
            ).start()
        return carry

    lax.fori_loop(0, total, start, 0)
    for which, out in enumerate((cache_keys, cache_values)):
        pltpu.make_async_copy(out, out, sem.at[which]).wait()


def ordered(arrived, source):
    total = source.shape[0]
    shape = (1, total) + arrived.shape[3:]
    spec = pl.BlockSpec(shape, lambda i, source: (0, 0, 0, 0))
    result = jax.ShapeDtypeStruct(shape, arrived.dtype)
    return pl.pallas_call(
        order_kernel,
        grid_spec=pltpu.PrefetchScalarGridSpec(
            num_scalar_prefetch=1,
            grid=(1,),
            in_specs=[pl.BlockSpec(memory_space=pl.ANY)],
            out_specs=[spec, spec],
            scratch_shapes=[pltpu.SemaphoreType.DMA((2,))],
        ),
        out_shape=[result, result],
    )(source, arrived)


def attend_kernel(info, q, *refs):
    key_refs, value_refs, out = refs[:5], refs[5:10], refs[10]
    odd = info[0] == 1

    def block_of(group, index, lanes):
        far, two, swapped, near, own = group
        lo, hi = slice(0, BLOCK), slice(BLOCK, 2 * BLOCK)
        rows = hi if index % 2 == 0 else lo
        if index == 0:
            return jnp.where(odd, swapped[hi, lanes], far[:, lanes])
        if index <= 2:
            return two[rows, lanes]
        if index <= 4:
            return jnp.where(odd, near[rows, lanes], swapped[rows, lanes])
        return own[rows, lanes]

    row = lax.broadcasted_iota(jnp.int32, (BLOCK, BLOCK), 0)
    col = lax.broadcasted_iota(jnp.int32, (BLOCK, BLOCK), 1)
    scale = HEAD_DIM ** (-0.5) * 1.4426950408889634

    def one(head, query_block, prior):
        lanes = slice(head * HEAD_DIM, (head + 1) * HEAD_DIM)
        rows = slice(query_block * BLOCK, (query_block + 1) * BLOCK)
        last = MAXB - 1 + query_block
        valid = info[3 + query_block]
        query = q[rows, lanes]
        window = range(last - prior, last + 1)
        parts = [
            lax.dot_general(
                query,
                block_of(key_refs, j, lanes),
                (((1,), (1,)), ((), ())),
                preferred_element_type=jnp.float32,
            )
            for j in window
        ]
        parts[-1] = jnp.where((col <= row) & (col < valid), parts[-1], MASKED_SCORE)
        best = parts[0]
        for part in parts[1:]:
            best = jnp.maximum(best, part)
        peak = jnp.max(best, axis=1, keepdims=True)
        weights = [jnp.exp2((part - peak) * scale) for part in parts]
        summed = weights[0]
        for part in weights[1:]:
            summed = summed + part
        totals = jnp.sum(summed, axis=1, keepdims=True)
        mixed = jnp.zeros((BLOCK, HEAD_DIM), jnp.float32)
        for j, part in zip(window, weights):
            mixed = mixed + jnp.dot(
                part.astype(jnp.bfloat16),
                block_of(value_refs, j, lanes),
                preferred_element_type=jnp.float32,
            )
        result = jnp.where(row < valid, mixed / totals, 0.0)
        out[rows, lanes] = result.astype(jnp.bfloat16)

    for query_block in range(2):
        for prior in range(MAXB):

            @pl.when(info[1 + query_block] == prior)
            def _():
                for head in range(HEADS_STEP):
                    one(head, query_block, prior)


def attend(info, queries, key_parts, value_parts):
    width = HEADS_STEP * HEAD_DIM
    tokens_here, features = queries.shape
    half = tokens_here // 2
    whole = pl.BlockSpec((tokens_here, width), lambda h, info: (0, h))
    far = pl.BlockSpec((half, width), lambda h, info: (0, h * (1 - info[0])))
    near = pl.BlockSpec((tokens_here, width), lambda h, info: (0, h * info[0]))
    group = [far, whole, whole, near, whole]
    return pl.pallas_call(
        attend_kernel,
        grid_spec=pltpu.PrefetchScalarGridSpec(
            num_scalar_prefetch=1,
            grid=(features // width,),
            in_specs=[whole] + group + group,
            out_specs=whole,
        ),
        out_shape=jax.ShapeDtypeStruct(queries.shape, jnp.bfloat16),
        cost_estimate=pl.CostEstimate(
            flops=4 * tokens_here * MAXB * BLOCK * features,
            transcendentals=0,
            bytes_accessed=10 * tokens_here * features,
        ),
    )(info, queries, *key_parts, *value_parts)


def window_parts(own, devices):
    by_two = [(i, i + 2) for i in range(devices - 2)]
    by_three = [(i, i + 3) for i in range(1, devices - 3, 2)]
    to_odd = [(i, i + 1) for i in range(0, devices, 2)]
    exchange = [(i, i ^ 1) for i in range(devices)]
    two = sent(own, by_two)
    far = sent(own[BLOCK:], by_three)
    near = sent(own, to_odd)
    swapped = sent(two, exchange)
    return [far, two, swapped, near, own]


def program(queries, keys, values, block_counts, last_tokens, pack_order, decode_slot):
    devices = lax.axis_size("seq")
    own_index = lax.axis_index("seq")
    blocks_here = queries.shape[0] // BLOCK
    assert blocks_here == 2 and devices % 2 == 0
    splits = devices // HEADS
    within, valid_tokens, source = block_tables(
        block_counts, last_tokens, pack_order, decode_slot, blocks_here * devices, BLOCK
    )
    key_parts = window_parts(keys, devices)
    value_parts = window_parts(values, devices)
    outgoing = packed(keys, values, splits)
    arrived = lax.all_to_all(outgoing, "seq", split_axis=0, concat_axis=0, tiled=True)
    first = own_index * blocks_here
    info = jnp.concatenate(
        [
            (own_index % 2)[None].astype(jnp.int32),
            lax.dynamic_slice_in_dim(within, first, blocks_here),
            lax.dynamic_slice_in_dim(valid_tokens, first, blocks_here),
        ]
    )
    attended = attend(info, queries, key_parts, value_parts)
    cache_keys, cache_values = ordered(arrived, source)
    return (attended, cache_keys, cache_values)


def solution(mesh):
    placed = (
        P(("groups", "seq"), None),
        P(("groups", "seq"), None),
        P(("groups", "seq"), None),
        P("groups"),
        P("groups"),
        P("groups"),
        P("groups"),
    )
    return jax.shard_map(
        program,
        mesh=mesh,
        in_specs=placed,
        out_specs=(
            P(("groups", "seq"), None),
            P(("groups", "seq"), None, None, None),
            P(("groups", "seq"), None, None, None),
        ),
        check_vma=False,
    )
```
